256 devices in a mesh: tm: 64 (over x, z, core), lev: 4 (over y).
Axes of the slice: x: 4, y: 4, z: 8, core: 2. Of those that a mesh axis runs over, the one named last changes fastest.
Arguments:
- fields: bfloat16 [4, 256, 72, 16384], P('lev', 'tm'), may hold values from -18 to 18
- lengths: int32 [64], P('tm'), may hold values from 1 to 4, 192 in all
- owners: int32 [72], replicated, may hold values from 0 to 63, as said below
- thickness: float32 [4], replicated, may hold values from 0.2 to 5
Outputs:
- daily_means: float32 [4, 128, 8, 16384], P('lev', 'tm')
- column_means: float32 [128, 8, 16384], P('tm', None, 'lev')
The draws below stay inside these ranges and needn't reach their ends.
Inputs may be any that keep to these rules, and one draw needn't show every extreme that they name: `lengths`: the entries sum to 192 and the largest is exactly 4. `owners`: no index owns more than 2 tiles; some index owns exactly 2.
All inputs are finite; a program needn't handle non-finite values. No bound on the sum of `lengths` on one device may be relied on, other than what follows from the above.
Results may differ from the reference program's by a relative error of at most 0.0003.
Values may be sent and summed in bfloat16 or wider, within the bound.
A program may use at most 128 MiB of HBM per device.

```python
import math
import jax
import jax.numpy as jnp
import numpy as np
from jax import lax

CELLS = 16384
MAXT = 2
CAP = 4
TILES = 72
STEPS = 192
DAYS = 8
LEVELS = 4
N_TM = 64


def draw_owners(key, part):
    shuffled = jax.random.permutation(key, MAXT * N_TM)
    return (shuffled[:TILES] % N_TM).astype(jnp.int32)


def block_scale(rng, dims, pieces, smallest, top_value):
    factor_of, own = 1.0, jax.random.fold_in(rng, 6)
    for axis_at, blocks in pieces:
        heights = jnp.exp(jax.random.uniform(jax.random.fold_in(own, axis_at), (blocks,), jnp.float32, smallest / len(pieces), top_value / len(pieces)))
        factor_of = factor_of * jnp.repeat(heights, dims[axis_at] // blocks).reshape([-1 if axis == axis_at else 1 for axis in range(len(dims))])
    return factor_of


def profile(number_of, total, bound, lean):
    loads = [(1 << 20) // math.isqrt(grade ** lean) + 1 for grade in range(2, number_of + 1)]
    rest, counts = total - bound - (number_of - 1), [1] * (number_of - 1)
    while rest > 0:
        movable = [i for i in range(number_of - 1) if counts[i] < bound]
        mass, left = sum([loads[i] for i in movable]), rest
        for i in movable:
            more = min(bound - counts[i], max(1, left * loads[i] // mass), rest)
            counts[i] = counts[i] + more
            rest = rest - more
    return np.array([bound] + counts)


def ragged_sizes(own_key, count, total, reach, slope):
    if count == 2:
        one = jax.random.randint(own_key, (), max(1, total - reach), min(reach, total - 1) + 1)
        return jnp.stack([one, total - one])
    sizes = jnp.asarray(profile(count, total, reach, slope), jnp.int32)
    twos = (count - 1) // 2
    donor, sink = sizes[1:1 + 2 * twos:2], sizes[2:2 + 2 * twos:2]
    slack = jnp.minimum(donor - 1, reach - sink)
    shifted = jax.random.randint(jax.random.fold_in(own_key, 1), (twos,), 0, 1 << 20) % (slack + 1)
    sizes = sizes.at[1:1 + 2 * twos:2].set(donor - shifted).at[2:2 + 2 * twos:2].set(sink + shifted)
    return sizes[jax.random.permutation(jax.random.fold_in(own_key, 2), count)]


def noise(own_key, shape, spread, reach, cuts=(), held_as=jnp.bfloat16):
    array = spread * jax.random.normal(own_key, shape, jnp.float32)
    if cuts:
        array = array * block_scale(own_key, shape, cuts, -0.22, 0.18)
    return jnp.clip(array, -reach, reach).astype(held_as)


def setup_inputs(seed: int = 0) -> dict:
    streams_of = jax.random.split(jax.random.key(seed), 5)
    fields = noise(streams_of[0], (LEVELS, N_TM * CAP, TILES, CELLS), 3.0, 18.0, ((0, 4), (1, 64)))
    lengths = ragged_sizes(streams_of[1], N_TM, STEPS, CAP, 2).astype(jnp.int32)
    owners = draw_owners(jax.random.fold_in(streams_of[4], 71), 0)
    thickness = jnp.clip(jnp.exp(jax.random.uniform(streams_of[3], (LEVELS,), jnp.float32, math.log(0.2), math.log(5.0))), 0.2, 5.0)
    return {"fields": fields, "lengths": lengths, "owners": owners, "thickness": thickness}


def slot_table(owners):
    tile_count = owners.shape[0]
    tile_ids = jnp.arange(tile_count, dtype=jnp.int32)
    earlier = (owners[None, :] == owners[:, None]) & (tile_ids[None, :] < tile_ids[:, None])
    tile_rank = jnp.sum(earlier.astype(jnp.int32), axis=1).astype(jnp.int32)
    position = (owners * MAXT + tile_rank).astype(jnp.int32)
    slot_ids = jnp.arange(N_TM * MAXT, dtype=jnp.int32)
    matches = (position[None, :] == slot_ids[:, None]).astype(jnp.int32)
    tile_of = jnp.sum(matches * tile_ids[None, :], axis=1).astype(jnp.int32)
    slot_valid = jnp.sum(matches, axis=1).astype(jnp.int32)
    return tile_of, slot_valid


def reference(fields, lengths, owners, thickness):
    offsets = (jnp.cumsum(lengths) - lengths).astype(jnp.int32)
    row_ids = jnp.arange(N_TM * CAP, dtype=jnp.int32)
    source_ids = row_ids // CAP
    slot_ids = row_ids % CAP
    hour_of = offsets[source_ids] + slot_ids
    is_valid = slot_ids < lengths[source_ids]
    day_ids = jnp.arange(DAYS, dtype=jnp.int32)
    select = (is_valid[:, None] & (hour_of[:, None] // 24 == day_ids[None, :])).astype(jnp.bfloat16)
    tile_of, slot_valid = slot_table(owners)
    keep = slot_valid.astype(jnp.float32)[:, None, None] / 24.0

    def level_means(level_fields):
        flat = level_fields.reshape(N_TM * CAP, TILES * CELLS)
        day_sums = jnp.dot(select.T, flat, preferred_element_type=jnp.float32)
        day_sums = day_sums.reshape(DAYS, TILES, CELLS)
        picked = jnp.take(day_sums, tile_of, axis=1)
        return jnp.transpose(picked, (1, 0, 2)) * keep

    daily_means = lax.map(level_means, fields)
    fraction = thickness / jnp.sum(thickness)
    column_means = jnp.sum(fraction[:, None, None, None] * daily_means, axis=0)
    return daily_means, column_means
```

```python
import jax
import jax.numpy as jnp
from jax import lax
from jax.experimental import pallas as pl
from jax.experimental.pallas import tpu as pltpu
from jax.sharding import PartitionSpec as P

MESH = pl.DeviceIdType.MESH
MAXT = 2
CAP = 4
TILES = 72
CELLS = 16384
NX, NZ, NC, NY = 4, 8, 2, 4
N_TM = NX * NZ * NC
DAYS = 8
CH = CELLS // (NZ * NC)
HALF = CELLS // NC
GROUPS = TILES // 8
XSLOTS = 4
ZW = GROUPS * CH + 128
FW = CH + 128
TOP = 32700.0
FINE = 256.0


def far_first(n):
    k = (n + 1) // 2
    return lax.rem(4 + k * (2 * lax.rem(n, 2) - 1) + 8, 8)


def code_of(peak):
    return jnp.ceil(jnp.log(jnp.maximum(peak, 1e-30)) * FINE)


def kernel(fields, wz, cz, frac, pick, spread, daily, column,
           own, other, zf32, zbuf, acc, fbuf, lsend, lrecv,
           own_sem, pair_send, pair_recv, z_send, z_recv, f_send, f_recv, l_send, l_recv):
    me = lax.axis_index("tm")
    my_y = lax.axis_index("lev")
    core = lax.rem(me, NC)
    my_z = lax.rem(me // NC, NZ)
    my_x = me // (NC * NZ)
    partner = me + 1 - 2 * core

    def own_copy(n):
        lanes = pl.multiple_of(core * HALF + lax.rem(my_z + far_first(n), NZ) * CH, CH)
        return pltpu.make_async_copy(
            fields.at[0, :, :, pl.ds(lanes, CH)], own.at[n], own_sem.at[n])

    def pair_copy(n):
        lanes = pl.multiple_of((1 - core) * HALF + lax.rem(my_z + far_first(n), NZ) * CH, CH)
        return pltpu.make_async_remote_copy(
            src_ref=fields.at[0, :, :, pl.ds(lanes, CH)], dst_ref=other.at[n],
            send_sem=pair_send.at[n], recv_sem=pair_recv.at[n],
            device_id=(partner, my_y), device_id_type=MESH)

    def start_own(n, carry):
        own_copy(n).start()
        return carry

    lax.fori_loop(0, NZ, start_own, 0)

    barrier = pltpu.get_barrier_semaphore()

    def greet_tm(r, carry):
        pl.semaphore_signal(barrier, inc=1, device_id=(lax.rem(me + r, N_TM), my_y), device_id_type=MESH)
        return carry

    def greet_lev(r, carry):
        pl.semaphore_signal(barrier, inc=1, device_id=(me, lax.rem(my_y + r, NY)), device_id_type=MESH)
        return carry

    lax.fori_loop(1, N_TM, greet_tm, 0)
    lax.fori_loop(1, NY, greet_lev, 0)
    pl.semaphore_wait(barrier, N_TM - 1 + NY - 1)

    def start_pair(n, carry):
        pair_copy(n).start()
        return carry

    lax.fori_loop(0, NZ, start_pair, 0)

    def z_copy(off):
        target = (my_x * NZ + lax.rem(my_z + off, NZ)) * NC + core
        return pltpu.make_async_remote_copy(
            src_ref=zbuf.at[off], dst_ref=zbuf.at[NZ + off],
            send_sem=z_send.at[off], recv_sem=z_recv.at[off],
            device_id=(target, my_y), device_id_type=MESH)

    def z_out(n, carry):
        off = far_first(n)
        own_copy(n).wait()
        pair_copy(n).wait_recv()

        def sums(g, peak):
            rows = pl.ds(pl.multiple_of(g * 8, 8), 8)
            first = jnp.zeros((8, CH), jnp.float32)
            second = jnp.zeros((8, CH), jnp.float32)
            for part, ref in enumerate((own, other)):
                for j in range(CAP):
                    hour = ref[n, j, rows, :].astype(jnp.float32)
                    first += wz[part * 8 + j] * hour
                    second += wz[part * 8 + 4 + j] * hour
            zf32[g, 0:8, :] = first
            zf32[g, 8:16, :] = second
            both = jnp.concatenate([first, second], axis=0)
            for l in range(CH // 128):
                peak = jnp.maximum(peak, jnp.abs(both[:, l * 128:(l + 1) * 128]))
            return peak

        code = code_of(lax.fori_loop(0, GROUPS, sums, jnp.zeros((16, 128), jnp.float32)))
        scale = jnp.exp(code * (-1.0 / FINE)) * TOP
        zbuf[off, :, GROUPS * CH:] = code.astype(jnp.int32).astype(jnp.int16)

        def shrink(g, carry):
            for l in range(CH // 128):
                value = jnp.round(zf32[g, :, l * 128:(l + 1) * 128] * scale)
                at = pl.multiple_of(g * CH + l * 128, 128)
                zbuf[off, :, pl.ds(at, 128)] = value.astype(jnp.int32).astype(jnp.int16)
            return carry

        lax.fori_loop(0, GROUPS, shrink, 0)

        @pl.when(off > 0)
        def _():
            z_copy(off).start()

        return carry

    lax.fori_loop(0, NZ, z_out, 0)

    acc[...] = jnp.zeros_like(acc)

    def z_in(n, carry):
        off = far_first(n)

        @pl.when(off > 0)
        def _():
            z_copy(off).wait_recv()

        at = off + NZ * jnp.minimum(off, 1)
        code = zbuf[at, :, GROUPS * CH:].astype(jnp.int32).astype(jnp.float32)
        scale = jnp.exp(code * (1.0 / FINE)) * (1.0 / TOP)

        def add(g, carry):
            rows = pl.multiple_of(g * 8, 8)
            for l in range(CH // 128):
                lanes = pl.ds(pl.multiple_of(g * CH + l * 128, 128), 128)
                value = zbuf[at, :, lanes].astype(jnp.int32).astype(jnp.float32) * scale
                low, high = value[0:8], value[8:16]
                for s in range(XSLOTS):
                    here = (pl.ds(s * TILES + rows, 8), slice(l * 128, (l + 1) * 128))
                    acc[here] += cz[off * 8 + s] * low + cz[off * 8 + 4 + s] * high
            return carry

        lax.fori_loop(0, GROUPS, add, 0)
        return carry

    lax.fori_loop(0, NZ, z_in, 0)

    def owners_out(b, carry):
        lines = pick[pl.ds(pl.multiple_of(b * 64, 64), 64), :]
        for l in range(CH // 256):
            part = acc[:, l * 256:(l + 1) * 256]
            high = part.astype(jnp.bfloat16)
            rest = part - high.astype(jnp.float32)
            mid = rest.astype(jnp.bfloat16)
            low = (rest - mid.astype(jnp.float32)).astype(jnp.bfloat16)
            got = jnp.dot(lines, high, preferred_element_type=jnp.float32)
            got += jnp.dot(lines, mid, preferred_element_type=jnp.float32)
            got += jnp.dot(lines, low, preferred_element_type=jnp.float32)
            zf32[0:4, :, l * 256:(l + 1) * 256] = got.reshape(4, 16, 256)

        for t in range(8):
            rows = zf32[t // 2, (t % 2) * 8:(t % 2) * 8 + 8, 0:CH]
            peak = jnp.zeros((8, 128), jnp.float32)
            for l in range(CH // 128):
                peak = jnp.maximum(peak, jnp.abs(rows[:, l * 128:(l + 1) * 128]))
            code = code_of(peak)
            scale = jnp.exp(code * (-1.0 / FINE)) * TOP
            fbuf[b * 8 + t, :, CH:] = code.astype(jnp.int32).astype(jnp.int16)
            for l in range(CH // 128):
                value = jnp.round(rows[:, l * 128:(l + 1) * 128] * scale)
                fbuf[b * 8 + t, :, l * 128:(l + 1) * 128] = value.astype(jnp.int32).astype(jnp.int16)
        return carry

    lax.fori_loop(0, N_TM // 8, owners_out, 0)

    def relative(i):
        n, dc, dx = i // 8, lax.rem(i // 4, 2), lax.rem(i, 4)
        return dx, far_first(n), dc

    def f_copy(i):
        dx, dz, dc = relative(i)
        target = (lax.rem(my_x + dx, NX) * NZ + lax.rem(my_z + dz, NZ)) * NC + lax.rem(core + dc, NC)
        return pltpu.make_async_remote_copy(
            src_ref=fbuf.at[target], dst_ref=fbuf.at[N_TM + i],
            send_sem=f_send.at[i], recv_sem=f_recv.at[i],
            device_id=(target, my_y), device_id_type=MESH)

    SELF = N_TM - 8

    def f_start(i, carry):
        @pl.when(i != SELF)
        def _():
            f_copy(i).start()

        return carry

    lax.fori_loop(0, N_TM, f_start, 0)

    def l_copy(piece, to, turn):
        return pltpu.make_async_remote_copy(
            src_ref=lsend.at[piece], dst_ref=lrecv.at[turn, lax.rem(piece, 4)],
            send_sem=l_send.at[piece], recv_sem=l_recv.at[turn, lax.rem(piece, 4)],
            device_id=(me, to), device_id_type=MESH)

    def owners_in(p, carry):
        _, dz, dc = relative(p * 4)
        piece = lax.rem(core + dc, NC) * NZ + lax.rem(my_z - dz + NZ, NZ)
        parts = []
        for dx in range(NX):
            i = p * 4 + dx
            if dx == 0:
                @pl.when(i != SELF)
                def _():
                    f_copy(i).wait_recv()

                alone = jnp.where(i == SELF, 1, 0)
                at = alone * me + (1 - alone) * (N_TM + i)
            else:
                f_copy(i).wait_recv()
                at = N_TM + i
            code = fbuf[at, :, CH:].astype(jnp.int32).astype(jnp.float32)
            scale = jnp.exp(code * (1.0 / FINE)) * (1.0 / TOP)
            value = fbuf[at, :, 0:CH].astype(jnp.int32).astype(jnp.float32)
            parts.append(value * jnp.concatenate([scale] * (CH // 128), axis=1))
        value = jnp.concatenate(parts, axis=0)
        means = jnp.dot(spread[...], value, preferred_element_type=jnp.float32,
                        precision=lax.Precision.HIGHEST) * (1.0 / 24.0)
        lanes = pl.ds(pl.multiple_of(piece * CH, CH), CH)
        daily[0, 0, :, lanes] = means[0:8]
        daily[0, 1, :, lanes] = means[8:16]
        lsend[piece] = means * frac[0]
        to = piece // 4
        turn = lax.rem(to - my_y + NY, NY)

        @pl.when(turn > 0)
        def _():
            l_copy(piece, to, turn).start()

        return carry

    lax.fori_loop(0, NZ * NC, owners_in, 0)

    for s in range(4):
        total = lsend[my_y * 4 + s]
        for turn in range(1, NY):
            l_copy(my_y * 4 + s, my_y, turn).wait_recv()
            total += lrecv[turn, s]
        column[0, :, s * CH:(s + 1) * CH] = total[0:8]
        column[1, :, s * CH:(s + 1) * CH] = total[8:16]

    def drain_pair(n, carry):
        pair_copy(n).wait_send()
        return carry

    def drain_z(off, carry):
        z_copy(off).wait_send()
        return carry

    def drain_f(i, carry):
        @pl.when(i != SELF)
        def _():
            f_copy(i).wait_send()

        return carry

    def drain_l(piece, carry):
        to = piece // 4
        turn = lax.rem(to - my_y + NY, NY)

        @pl.when(turn > 0)
        def _():
            l_copy(piece, to, turn).wait_send()

        return carry

    lax.fori_loop(0, NZ, drain_pair, 0)
    lax.fori_loop(1, NZ, drain_z, 0)
    lax.fori_loop(0, N_TM, drain_f, 0)
    lax.fori_loop(0, NZ * NC, drain_l, 0)


def slot_table(owners, slot_total):
    tile_count = owners.shape[0]
    tile_ids = jnp.arange(tile_count, dtype=jnp.int32)
    earlier = (owners[None, :] == owners[:, None]) & (tile_ids[None, :] < tile_ids[:, None])
    tile_rank = jnp.sum(earlier.astype(jnp.int32), axis=1)
    return owners * MAXT + tile_rank


def local(fields, lengths, owners, thickness):
    me = lax.axis_index("tm")
    core, my_z, my_x = me % NC, (me // NC) % NZ, me // (NC * NZ)
    chip = me // NC
    lens = lax.all_gather(lengths, "tm", axis=0, tiled=True)
    ids = jnp.arange(N_TM, dtype=jnp.int32)
    offsets = jnp.sum(jnp.where(ids[None, :] < ids[:, None], lens[None, :], 0), axis=1)
    chip_day = offsets[::NC] // 24
    plane_day = offsets[:: NC * NZ] // 24
    devs = jnp.stack([me, me + 1 - 2 * core])
    j = jnp.arange(CAP, dtype=jnp.int32)
    slot = (offsets[devs][:, None] + j[None, :]) // 24 - chip_day[chip]
    slot = jnp.where(j[None, :] < lens[devs][:, None], slot, -1)
    wz = (slot[:, None, :] == jnp.arange(2)[None, :, None]).astype(jnp.float32).reshape(16)
    from_z = (my_z - jnp.arange(NZ) + NZ) % NZ
    shift = chip_day[my_x * NZ + from_z] - plane_day[my_x]
    cz = (shift[:, None, None] + jnp.arange(2)[None, :, None] == jnp.arange(XSLOTS)[None, None, :])
    cz = cz.astype(jnp.float32).reshape(NZ * 2 * XSLOTS)
    from_x = (my_x - jnp.arange(NX) + NX) % NX
    rows, cols = jnp.arange(16, dtype=jnp.int32), jnp.arange(32, dtype=jnp.int32)
    day = plane_day[from_x][cols // 8] + cols % 4
    spread = (rows[:, None] // 8 == ((cols // 4) % 2)[None, :]) & (rows[:, None] % 8 == day[None, :])
    spread = spread.astype(jnp.float32)
    position = slot_table(owners, N_TM * MAXT)
    lines = jnp.arange(N_TM * MAXT * XSLOTS, dtype=jnp.int32)
    taken = (position[None, :] == (lines // XSLOTS)[:, None])
    pick = jnp.concatenate(
        [taken & (lines % XSLOTS == s)[:, None] for s in range(XSLOTS)], axis=1).astype(jnp.bfloat16)
    frac = (thickness[lax.axis_index("lev")] / jnp.sum(thickness)).reshape(1)

    dma = pltpu.SemaphoreType.DMA
    daily, column = pl.pallas_call(
        kernel,
        out_shape=(
            jax.ShapeDtypeStruct((1, MAXT, DAYS, CELLS), jnp.float32),
            jax.ShapeDtypeStruct((MAXT, DAYS, CELLS // NY), jnp.float32),
        ),
        in_specs=[
            pl.BlockSpec(memory_space=pl.ANY),
            pl.BlockSpec(memory_space=pltpu.SMEM),
            pl.BlockSpec(memory_space=pltpu.SMEM),
            pl.BlockSpec(memory_space=pltpu.SMEM),
            pl.BlockSpec(memory_space=pltpu.VMEM),
            pl.BlockSpec(memory_space=pltpu.VMEM),
        ],
        out_specs=(pl.BlockSpec(memory_space=pltpu.VMEM), pl.BlockSpec(memory_space=pltpu.VMEM)),
        scratch_shapes=[
            pltpu.VMEM((NZ, CAP, TILES, CH), jnp.bfloat16),
            pltpu.VMEM((NZ, CAP, TILES, CH), jnp.bfloat16),
            pltpu.VMEM((GROUPS, 16, CH), jnp.float32),
            pltpu.VMEM((2 * NZ, 16, ZW), jnp.int16),
            pltpu.VMEM((XSLOTS * TILES, CH), jnp.float32),
            pltpu.VMEM((2 * N_TM, 8, FW), jnp.int16),
            pltpu.VMEM((NZ * NC, 16, CH), jnp.float32),
            pltpu.VMEM((NY, 4, 16, CH), jnp.float32),
            dma((NZ,)), dma((NZ,)), dma((NZ,)), dma((NZ,)), dma((NZ,)),
            dma((N_TM,)), dma((N_TM,)), dma((NZ * NC,)), dma((NY, 4)),
        ],
        compiler_params=pltpu.CompilerParams(collective_id=0, has_side_effects=True),
    )(fields, wz, cz, frac, pick, spread)
    return daily, column


def solution(mesh):
    placed = (P("lev", "tm", None, None), P("tm"), P(), P())
    return jax.shard_map(
        local,
        mesh=mesh,
        in_specs=placed,
        out_specs=(P("lev", "tm", None, None), P("tm", None, "lev")),
        check_vma=False,
    )
```

```python
import jax
import jax.numpy as jnp
from jax import lax
from jax.experimental import pallas as pl
from jax.experimental.pallas import tpu as pltpu
from jax.sharding import PartitionSpec as P

MESH = pl.DeviceIdType.MESH
MAXT = 2
CAP = 4
TILES = 72
CELLS = 16384
NX, NZ, NC, NY = 4, 8, 2, 4
N_TM = NX * NZ * NC
CHIPS = NX * NZ
DAYS = 8
CH = CELLS // (NZ * NC)
HALF = CELLS // NC
GROUPS = TILES // 8
WIN = 4
SUB = 2
CW = CH // SUB
LONG, SHORT = 4, 3
FW = CH + 128
TOP = 32700.0
FINE = 256.0


def touched(chips):
    return (8 * chips - 2) // 24 + 2


def far_first(n):
    k = (n + 1) // 2
    return lax.rem(4 + k * (2 * lax.rem(n, 2) - 1) + 8, 8)


def code_of(peak):
    return jnp.ceil(jnp.log(jnp.maximum(peak, 1e-30)) * FINE)


def day_of(hour):
    return lax.shift_right_logical(hour * 2731, 16)


def kernel(fields, length, thickness, place, daily, column,
           own, other, lens, offs, pick, zf32, two_out, two_in, three_out, three_in, acc, fbuf, lsend, lrecv,
           own_sem, pair_send, pair_recv, n_send, n_recv, z_send, z_recv, f_send, f_recv, l_send, l_recv):
    me = lax.axis_index("tm")
    my_y = lax.axis_index("lev")
    core = lax.rem(me, NC)
    chip = me // NC
    my_z = lax.rem(chip, NZ)
    my_x = chip // NZ
    partner = me + 1 - 2 * core
    way = 1 - 2 * core

    def chunk_lanes(n, of_core):
        ahead = (1 - lax.rem(n, 2)) * (4 - n // 2) - lax.rem(n, 2) * (3 - n // 2)
        z = lax.rem(my_z + ahead * (1 - 2 * of_core) + NZ, NZ)
        return pl.ds(pl.multiple_of(of_core * HALF + z * CH, CH), CH)

    def own_copy(n):
        return pltpu.make_async_copy(
            fields.at[0, :, :, chunk_lanes(n, core)], own.at[n], own_sem.at[n])

    def pair_copy(n):
        return pltpu.make_async_remote_copy(
            src_ref=fields.at[0, :, :, chunk_lanes(n, 1 - core)], dst_ref=other.at[n],
            send_sem=pair_send.at[n], recv_sem=pair_recv.at[n],
            device_id=(partner, my_y), device_id_type=MESH)

    def start_own(n, carry):
        own_copy(n).start()
        return carry

    lax.fori_loop(0, NZ, start_own, 0)

    barrier = pltpu.get_barrier_semaphore()

    def greet_tm(r, carry):
        pl.semaphore_signal(barrier, inc=1, device_id=(lax.rem(me + r, N_TM), my_y), device_id_type=MESH)
        return carry

    def greet_lev(r, carry):
        pl.semaphore_signal(barrier, inc=1, device_id=(me, lax.rem(my_y + r, NY)), device_id_type=MESH)
        return carry

    lax.fori_loop(1, N_TM, greet_tm, 0)
    lax.fori_loop(1, NY, greet_lev, 0)

    lens[pl.ds(me, 1), :] = jnp.full((1, 128), length[0], jnp.int32)
    width = WIN * TILES
    line = lax.broadcasted_iota(jnp.int32, (MAXT * N_TM * WIN, width), 0)
    lane = lax.broadcasted_iota(jnp.int32, (MAXT * N_TM * WIN, width), 1)
    first_lane = (line & 3) * TILES
    taken = (place[...] == lax.shift_right_logical(line, 2)) & (lane >= first_lane) & (lane < first_lane + TILES)
    pick[...] = jnp.where(taken, 1.0, 0.0).astype(jnp.bfloat16)
    share = jnp.full((16, 128), thickness[my_y], jnp.float32) / jnp.full(
        (16, 128), thickness[0] + thickness[1] + thickness[2] + thickness[3], jnp.float32)

    pl.semaphore_wait(barrier, N_TM - 1 + NY - 1)

    def length_copy(r):
        return pltpu.make_async_remote_copy(
            src_ref=lens.at[pl.ds(me, 1), :], dst_ref=lens.at[pl.ds(me, 1), :],
            send_sem=n_send.at[r], recv_sem=n_recv.at[r],
            device_id=(lax.rem(me + r, N_TM), my_y), device_id_type=MESH)

    def start_length(r, carry):
        length_copy(r).start()
        return carry

    def start_pair(n, carry):
        pair_copy(n).start()
        return carry

    def take_length(r, carry):
        length_copy(r).wait_recv()
        return carry

    lax.fori_loop(0, 2, start_pair, 0)
    lax.fori_loop(1, N_TM, start_length, 0)
    lax.fori_loop(2, NZ, start_pair, 0)
    lax.fori_loop(1, N_TM, take_length, 0)
    before = (lax.broadcasted_iota(jnp.int32, (N_TM, N_TM), 1)
              < lax.broadcasted_iota(jnp.int32, (N_TM, N_TM), 0))
    offs[...] = jnp.dot(
        jnp.where(before, 1.0, 0.0).astype(jnp.bfloat16),
        lens[...].astype(jnp.float32).astype(jnp.bfloat16),
        preferred_element_type=jnp.float32).astype(jnp.int32)

    def day(q):
        q = lax.rem(q + 2 * CHIPS, CHIPS)
        return day_of(jnp.broadcast_to(offs[pl.ds(q * NC, 1), :], (8, 128)))

    my_day = day(chip)

    def hour_weights(device):
        start = jnp.broadcast_to(offs[pl.ds(device, 1), :], (8, 128))
        held = jnp.broadcast_to(lens[pl.ds(device, 1), :], (8, 128))
        slots = [jnp.where(held > j, day_of(start + j) - my_day, -1) for j in range(CAP)]
        return [[jnp.where(slot == i, 1.0, 0.0) for slot in slots] for i in range(2)]

    weights = (hour_weights(me), hour_weights(partner))

    def moves(shift, slots, total):
        return [[jnp.where(shift == s - i, 1.0, 0.0) if s >= i else None for s in range(total)] for i in range(slots)]

    def chip_sums(n, g, lanes):
        rows = pl.ds(pl.multiple_of(g * 8, 8), 8)
        sums = [None, None]
        for part, ref in enumerate((own, other)):
            for j in range(CAP):
                hour = ref[n, j, rows, lanes].astype(jnp.float32)
                for i in range(2):
                    term = weights[part][i][j] * hour
                    sums[i] = term if sums[i] is None else sums[i] + term
        return sums

    def scale_in(buf, units):
        code = buf[:, units * CW:].astype(jnp.int32).astype(jnp.float32)
        return jnp.exp(code * (1.0 / FINE)) * (1.0 / TOP)

    def taken_in(buf, unit, l, scale):
        lanes = pl.ds(pl.multiple_of(unit * CW + l * 128, 128), 128)
        return buf[:, lanes].astype(jnp.int32).astype(jnp.float32) * scale

    def combined(total, sources):
        outs = [None] * total
        for values, table in sources:
            for i, value in enumerate(values):
                for s in range(i, total):
                    term = table[i][s] * value
                    outs[s] = term if outs[s] is None else outs[s] + term
        return outs

    def link(short, n, s):
        at = n - 1 + (LONG if short else 0)
        if n == LONG:
            src, dst = three_out.at[s], three_in.at[s]
        else:
            row = n - 1 + (3 if short else 0)
            src, dst = two_out.at[row, s], two_in.at[row, s]
        to = lax.rem(chip + (-way if short else way) + CHIPS, CHIPS)
        return pltpu.make_async_remote_copy(
            src_ref=src, dst_ref=dst, send_sem=z_send.at[at, s], recv_sem=z_recv.at[at, s],
            device_id=(to * NC + core, my_y), device_id_type=MESH)

    def arrived(short, n, s):
        if n == LONG:
            return three_in.at[s]
        return two_in.at[n - 1 + (3 if short else 0), s]

    def forward(short, n):
        at = 2 * n - 1 if short else 2 * (n - 1)
        own_copy(at).wait()
        pair_copy(at).wait_recv()
        rising = core if short else 1 - core
        first = chip - (n - 1) * rising
        base = day(first)
        total = touched(n)
        mine = moves((my_day - base) & 7, 2, total)
        if n > 1:
            theirs = moves((day(first + 1 - rising) - base) & 7, 2, total)

        def part(s, carry):
            if n > 1:
                link(short, n - 1, s).wait_recv()
                source = arrived(short, n - 1, s)
                scale = scale_in(source, 2 * GROUPS)

            def sums(g, peak):
                for l in range(CW // 128):
                    lanes = pl.ds(pl.multiple_of(s * CW + l * 128, 128), 128)
                    sources = [(chip_sums(at, g, lanes), mine)]
                    if n > 1:
                        sources.append(([taken_in(source, i * GROUPS + g, l, scale) for i in range(2)], theirs))
                    for i, value in enumerate(combined(total, sources)):
                        zf32[i * GROUPS + g, :, l * 128:(l + 1) * 128] = value
                        peak = jnp.maximum(peak, jnp.abs(value))
                return peak

            code = code_of(lax.fori_loop(0, GROUPS, sums, jnp.zeros((8, 128), jnp.float32)))
            down = jnp.exp(code * (-1.0 / FINE)) * TOP
            out = three_out.at[s] if n == LONG else two_out.at[n - 1 + (3 if short else 0), s]
            out[:, total * GROUPS * CW:] = code.astype(jnp.int32).astype(jnp.int16)

            def shrink(u, carry):
                for l in range(CW // 128):
                    value = jnp.round(zf32[u, :, l * 128:(l + 1) * 128] * down)
                    lanes = pl.ds(pl.multiple_of(u * CW + l * 128, 128), 128)
                    out[:, lanes] = value.astype(jnp.int32).astype(jnp.int16)
                return carry

            lax.fori_loop(0, total * GROUPS, shrink, 0)
            link(short, n, s).start()
            return carry

        lax.fori_loop(0, SUB, part, 0)

    for n in range(1, LONG + 1):
        forward(False, n)
        if n <= SHORT:
            forward(True, n)

    own_copy(NZ - 1).wait()
    pair_copy(NZ - 1).wait_recv()
    base = day(chip - (LONG - core))
    mine = moves((my_day - base) & 7, 2, WIN)
    long_day = day(chip - LONG + core * (LONG + 1))
    short_day = day(chip + 1 - core * (SHORT + 1))
    from_long = moves((long_day - base) & 7, touched(LONG), WIN)
    from_short = moves((short_day - base) & 7, touched(SHORT), WIN)

    def window(s, carry):
        link(False, LONG, s).wait_recv()
        link(True, SHORT, s).wait_recv()
        far, near = arrived(False, LONG, s), arrived(True, SHORT, s)
        far_scale = scale_in(far, touched(LONG) * GROUPS)
        near_scale = scale_in(near, touched(SHORT) * GROUPS)

        def add(g, carry):
            for l in range(CW // 128):
                lanes = pl.ds(pl.multiple_of(s * CW + l * 128, 128), 128)
                outs = combined(WIN, [
                    (chip_sums(NZ - 1, g, lanes), mine),
                    ([taken_in(far, i * GROUPS + g, l, far_scale) for i in range(touched(LONG))], from_long),
                    ([taken_in(near, i * GROUPS + g, l, near_scale) for i in range(touched(SHORT))], from_short),
                ])
                for i, value in enumerate(outs):
                    acc[pl.ds(pl.multiple_of(i * TILES + g * 8, 8), 8), lanes] = value
            return carry

        lax.fori_loop(0, GROUPS, add, 0)
        return carry

    lax.fori_loop(0, SUB, window, 0)

    def owners_out(b, carry):
        lines = pick[pl.ds(pl.multiple_of(b * 64, 64), 64), :]
        for l in range(CH // 256):
            part = acc[:, l * 256:(l + 1) * 256]
            high = part.astype(jnp.bfloat16)
            rest = part - high.astype(jnp.float32)
            mid = rest.astype(jnp.bfloat16)
            low = (rest - mid.astype(jnp.float32)).astype(jnp.bfloat16)
            got = jnp.dot(lines, high, preferred_element_type=jnp.float32)
            got += jnp.dot(lines, mid, preferred_element_type=jnp.float32)
            got += jnp.dot(lines, low, preferred_element_type=jnp.float32)
            lsend[0:4, :, l * 256:(l + 1) * 256] = got.reshape(4, 16, 256)

        for t in range(8):
            rows = lsend[t // 2, (t % 2) * 8:(t % 2) * 8 + 8, :]
            peak = jnp.zeros((8, 128), jnp.float32)
            for l in range(CH // 128):
                peak = jnp.maximum(peak, jnp.abs(rows[:, l * 128:(l + 1) * 128]))
            code = code_of(peak)
            scale = jnp.exp(code * (-1.0 / FINE)) * TOP
            fbuf[b * 8 + t, :, CH:] = code.astype(jnp.int32).astype(jnp.int16)
            for l in range(CH // 128):
                value = jnp.round(rows[:, l * 128:(l + 1) * 128] * scale)
                fbuf[b * 8 + t, :, l * 128:(l + 1) * 128] = value.astype(jnp.int32).astype(jnp.int16)
        return carry

    lax.fori_loop(0, N_TM // 8, owners_out, 0)

    def relative(i):
        return lax.rem(i, 4), far_first(i // 8), lax.rem(i // 4, 2)

    def f_copy(i):
        dx, dz, dc = relative(i)
        target = (lax.rem(my_x + dx, NX) * NZ + lax.rem(my_z + dz, NZ)) * NC + lax.rem(core + dc, NC)
        return pltpu.make_async_remote_copy(
            src_ref=fbuf.at[target], dst_ref=fbuf.at[N_TM + i],
            send_sem=f_send.at[i], recv_sem=f_recv.at[i],
            device_id=(target, my_y), device_id_type=MESH)

    SELF = N_TM - 8

    def f_start(i, carry):
        @pl.when(i != SELF)
        def _():
            f_copy(i).start()

        return carry

    lax.fori_loop(0, N_TM, f_start, 0)

    def l_copy(piece, to, turn):
        return pltpu.make_async_remote_copy(
            src_ref=lsend.at[piece], dst_ref=lrecv.at[turn, lax.rem(piece, 4)],
            send_sem=l_send.at[piece], recv_sem=l_recv.at[turn, lax.rem(piece, 4)],
            device_id=(me, to), device_id_type=MESH)

    col = lax.broadcasted_iota(jnp.int32, (16, 128), 1)
    row = lax.broadcasted_iota(jnp.int32, (16, 128), 0)

    def owners_in(p, carry):
        _, dz, dc = relative(p * 4)
        from_z = lax.rem(my_z - dz + NZ, NZ)
        from_core = lax.rem(core + dc, NC)
        piece = from_core * NZ + from_z
        parts = []
        start = jnp.zeros((16, 128), jnp.int32)
        for dx in range(NX):
            i = p * 4 + dx
            if dx == 0:
                @pl.when(i != SELF)
                def _():
                    f_copy(i).wait_recv()

                alone = jnp.where(i == SELF, 1, 0)
                at = alone * me + (1 - alone) * (N_TM + i)
            else:
                f_copy(i).wait_recv()
                at = N_TM + i
            code = fbuf[at, :, CH:].astype(jnp.int32).astype(jnp.float32)
            scale = jnp.exp(code * (1.0 / FINE)) * (1.0 / TOP)
            value = fbuf[at, :, 0:CH].astype(jnp.int32).astype(jnp.float32)
            parts.append(value * jnp.concatenate([scale] * (CH // 128), axis=1))
            from_day = day(lax.rem(my_x - dx + NX, NX) * NZ + from_z - (LONG - from_core))
            start = jnp.where(lax.shift_right_logical(col, 3) == dx, jnp.concatenate([from_day] * 2, axis=0), start)
        same = (lax.shift_right_logical(col, 2) & 1) == lax.shift_right_logical(row, 3)
        spread = jnp.where(same & (((start + (col & 3)) & 7) == (row & 7)), 1.0, 0.0)[:, 0:32]
        value = jnp.concatenate(parts, axis=0)
        means = jnp.dot(spread, value, preferred_element_type=jnp.float32,
                        precision=lax.Precision.HIGHEST) * (1.0 / 24.0)
        lanes = pl.ds(pl.multiple_of(piece * CH, CH), CH)
        daily[0, 0, :, lanes] = means[0:8]
        daily[0, 1, :, lanes] = means[8:16]
        lsend[piece] = means * jnp.concatenate([share] * (CH // 128), axis=1)
        to = piece // 4
        turn = lax.rem(to - my_y + NY, NY)

        @pl.when(turn > 0)
        def _():
            l_copy(piece, to, turn).start()

        return carry

    lax.fori_loop(0, NZ * NC, owners_in, 0)

    for s in range(4):
        total = lsend[my_y * 4 + s]
        for turn in range(1, NY):
            l_copy(my_y * 4 + s, my_y, turn).wait_recv()
            total += lrecv[turn, s]
        column[0, :, s * CH:(s + 1) * CH] = total[0:8]
        column[1, :, s * CH:(s + 1) * CH] = total[8:16]

    def drain_pair(n, carry):
        pair_copy(n).wait_send()
        return carry

    def drain_length(r, carry):
        length_copy(r).wait_send()
        return carry

    def drain_f(i, carry):
        @pl.when(i != SELF)
        def _():
            f_copy(i).wait_send()

        return carry

    def drain_l(piece, carry):
        to = piece // 4
        turn = lax.rem(to - my_y + NY, NY)

        @pl.when(turn > 0)
        def _():
            l_copy(piece, to, turn).wait_send()

        return carry

    lax.fori_loop(0, NZ, drain_pair, 0)
    lax.fori_loop(1, N_TM, drain_length, 0)
    for s in range(SUB):
        for n in range(1, LONG + 1):
            link(False, n, s).wait_send()
        for n in range(1, SHORT + 1):
            link(True, n, s).wait_send()
    lax.fori_loop(0, N_TM, drain_f, 0)
    lax.fori_loop(0, NZ * NC, drain_l, 0)


def slot_of(owners):
    ids = jnp.arange(TILES, dtype=jnp.int32)
    earlier = (owners[None, :] == owners[:, None]) & (ids[None, :] < ids[:, None])
    return owners * MAXT + jnp.sum(earlier.astype(jnp.int32), axis=1)


def local(fields, lengths, owners, thickness):
    place = jnp.tile(slot_of(owners), WIN)[None, :]
    dma = pltpu.SemaphoreType.DMA
    steps = LONG + SHORT
    two, three = 2 * GROUPS * CW + 128, 3 * GROUPS * CW + 128
    return pl.pallas_call(
        kernel,
        out_shape=(
            jax.ShapeDtypeStruct((1, MAXT, DAYS, CELLS), jnp.float32),
            jax.ShapeDtypeStruct((MAXT, DAYS, CELLS // NY), jnp.float32),
        ),
        in_specs=[
            pl.BlockSpec(memory_space=pl.ANY),
            pl.BlockSpec(memory_space=pltpu.SMEM),
            pl.BlockSpec(memory_space=pltpu.SMEM),
            pl.BlockSpec(memory_space=pltpu.VMEM),
        ],
        out_specs=(pl.BlockSpec(memory_space=pltpu.VMEM), pl.BlockSpec(memory_space=pltpu.VMEM)),
        scratch_shapes=[
            pltpu.VMEM((NZ, CAP, TILES, CH), jnp.bfloat16),
            pltpu.VMEM((NZ, CAP, TILES, CH), jnp.bfloat16),
            pltpu.VMEM((N_TM, 128), jnp.int32),
            pltpu.VMEM((N_TM, 128), jnp.int32),
            pltpu.VMEM((MAXT * N_TM * WIN, WIN * TILES), jnp.bfloat16),
            pltpu.VMEM((3 * GROUPS, 8, CW), jnp.float32),
            pltpu.VMEM((6, SUB, 8, two), jnp.int16),
            pltpu.VMEM((6, SUB, 8, two), jnp.int16),
            pltpu.VMEM((SUB, 8, three), jnp.int16),
            pltpu.VMEM((SUB, 8, three), jnp.int16),
            pltpu.VMEM((WIN * TILES, CH), jnp.float32),
            pltpu.VMEM((2 * N_TM, 8, FW), jnp.int16),
            pltpu.VMEM((NZ * NC, 16, CH), jnp.float32),
            pltpu.VMEM((NY, 4, 16, CH), jnp.float32),
            dma((NZ,)), dma((NZ,)), dma((NZ,)), dma((N_TM,)), dma((N_TM,)),
            dma((steps, SUB)), dma((steps, SUB)),
            dma((N_TM,)), dma((N_TM,)), dma((NZ * NC,)), dma((NY, 4)),
        ],
        compiler_params=pltpu.CompilerParams(collective_id=0, has_side_effects=True),
    )(fields, lengths, thickness, place)


def solution(mesh):
    placed = (P("lev", "tm", None, None), P("tm"), P(), P())
    return jax.shard_map(
        local,
        mesh=mesh,
        in_specs=placed,
        out_specs=(P("lev", "tm", None, None), P("tm", None, "lev")),
        check_vma=False,
    )
```
